32 devices in a mesh: dp: 4 (over x, core), expert: 8 (over z, y).
Axes of the slice: x: 2, y: 2, z: 4, core: 2. Of those that a mesh axis runs over, the one named last changes fastest.
Arguments:
- tokens: bfloat16 [4096, 2048], P(('dp', 'expert')), may hold values from -6 to 6
- norm_gain: bfloat16 [2048], replicated, may hold values from 0.099609375 to 1.8984375
- router_weight: bfloat16 [2048, 8], replicated, may hold values from -0.1875 to 0.1875
- w_gate: bfloat16 [8, 2048, 5120], P('expert', None, 'dp'), may hold values from -0.125 to 0.125
- w_up: bfloat16 [8, 2048, 5120], P('expert', None, 'dp'), may hold values from -0.125 to 0.125
- w_down: bfloat16 [8, 5120, 2048], P('expert', 'dp'), may hold values from -0.078125 to 0.078125
- selected: int32 [8, 896], replicated, may hold values from 0 to 4095, as said below
Outputs:
- combined: bfloat16 [4096, 2048], P(('dp', 'expert'))
The draws below stay inside these ranges and needn't reach their ends.
Inputs may be any that keep to these rules, and one draw needn't show every extreme that they name: `selected`: each row holds 896 distinct token indices in ascending order. Of one row's indices at most 64 fall among one device's 128 tokens and at most 336 among the tokens of one index of dp; every row reaches both bounds.
All inputs are finite; a program needn't handle non-finite values.
Results may differ from the reference program's by a relative error of at most 0.0072.
Values may be sent and summed in bfloat16 or wider, within the bound.
No kernel may reach another device: no remote copies, remote signals or barrier semaphores. Data moves between devices by JAX's collectives and lax.ppermute only.
A program may use at most 128 MiB of HBM per device.

```python
import jax
import jax.numpy as jnp
from jax import lax

D = 2048
FF = 5120
TOK_DEV = 128
EXPERTS = 8
TOKENS = 4096
CAP = 896
PEAK = 64
RMOST = 336
N_DP = 4
N_EXPERT = 8


def choose_tokens(key):
    keys = jax.random.split(key, 7)
    row_cells = N_DP * RMOST
    row_score = jax.random.randint(keys[0], (N_DP, RMOST), 0, 1024) + 1024 * jax.random.randint(keys[1], (N_DP, 1), 0, 16)
    forced_row = jax.random.randint(keys[2], (), 0, N_DP)
    row_score = row_score + jnp.where(jnp.arange(N_DP) == forced_row, 32768, 0)[:, None]
    row_distinct = row_score.reshape(-1) * row_cells + jnp.arange(row_cells)
    row_order = jnp.argsort(-row_distinct)
    row_ranks = jnp.argsort(row_order)
    row_counts = jnp.sum((row_ranks < CAP).reshape(N_DP, RMOST).astype(jnp.int32), axis=1)
    source_cells = N_EXPERT * PEAK
    source_score = jax.random.randint(keys[3], (N_DP, N_EXPERT, PEAK), 0, 1024) + 1024 * jax.random.randint(keys[4], (N_DP, N_EXPERT, 1), 0, 16)
    forced_source = jax.random.randint(keys[5], (N_DP,), 0, N_EXPERT)
    source_score = source_score + jnp.where(jnp.arange(N_EXPERT)[None, :] == forced_source[:, None], 32768, 0)[:, :, None]
    source_distinct = source_score.reshape(N_DP, source_cells) * source_cells + jnp.arange(source_cells)[None, :]
    source_order = jnp.argsort(-source_distinct, axis=1)
    source_ranks = jnp.argsort(source_order, axis=1)
    chosen_cells = source_ranks < row_counts[:, None]
    source_counts = jnp.sum(chosen_cells.reshape(N_DP, N_EXPERT, PEAK).astype(jnp.int32), axis=2).reshape(-1)
    shuffled = jnp.argsort(jax.random.randint(keys[6], (N_DP * N_EXPERT, TOK_DEV), 0, 1073741824), axis=1)[:, :PEAK]
    candidates = jnp.arange(N_DP * N_EXPERT)[:, None] * TOK_DEV + shuffled
    usable = jnp.arange(PEAK)[None, :] < source_counts[:, None]
    sort_keys = jnp.where(usable, candidates, N_DP * N_EXPERT * TOK_DEV).reshape(-1)
    return jnp.sort(sort_keys)[:CAP].astype(jnp.int32)


def draw_selected(key, part):
    expert_keys = jax.random.split(jax.random.fold_in(key, 17), EXPERTS)
    return jax.vmap(choose_tokens)(expert_keys)


def levels(key, dims, cuts, low, largest):
    gain, own = 1.0, jax.random.fold_in(key, 6)
    for axis_at, blocks in cuts:
        draws = jnp.exp(jax.random.uniform(jax.random.fold_in(own, axis_at), (blocks,), jnp.float32, low / len(cuts), largest / len(cuts)))
        gain = gain * jnp.repeat(draws, dims[axis_at] // blocks).reshape([-1 if axis == axis_at else 1 for axis in range(len(dims))])
    return gain


def normal_values(own_key, dims, width, bound, shards=(), dtype=jnp.bfloat16):
    values = jax.random.normal(own_key, dims, jnp.float32) * width
    if len(shards) > 0:
        values = levels(own_key, dims, shards, -0.22, 0.18) * values
    return jnp.clip(values, min=-bound, max=bound).astype(dtype)


def setup_inputs(seed: int = 0) -> dict:
    seeds = jax.random.split(jax.random.key(seed), 8)
    tokens = normal_values(seeds[0], (TOKENS, D), 1.0, 6.0, ((0, 32),))
    norm_gain = jnp.clip(1.0 + 0.18 * jax.random.normal(seeds[1], (D,), jnp.float32), 0.099609375, 1.8984375).astype(jnp.bfloat16)
    router_weight = normal_values(seeds[2], (D, EXPERTS), (D // 2) ** -0.5, 0.1875)
    w_gate = normal_values(seeds[3], (EXPERTS, D, FF), D ** -0.5, 0.125, ((0, 8), (2, 4)))
    w_up = normal_values(seeds[4], (EXPERTS, D, FF), D ** -0.5, 0.125, ((0, 8), (2, 4)))
    w_down = normal_values(seeds[5], (EXPERTS, FF, D), FF ** -0.5, 0.078125, ((0, 8), (1, 4)))
    selected = draw_selected(jax.random.fold_in(seeds[7], 71), 0)
    return dict(tokens=tokens, norm_gain=norm_gain, router_weight=router_weight, w_gate=w_gate, w_up=w_up, w_down=w_down, selected=selected)


def reference(tokens, norm_gain, router_weight, w_gate, w_up, w_down, selected):
    activations = tokens.astype(jnp.float32)
    mean_square = lax.optimization_barrier(jnp.mean(activations * activations, axis=1, keepdims=True))
    normed = (activations * lax.rsqrt(mean_square + 1e-06) * norm_gain.astype(jnp.float32)).astype(jnp.bfloat16)
    gate_probs = jax.nn.sigmoid(jnp.dot(normed, router_weight, preferred_element_type=jnp.float32))
    probs_by_expert = gate_probs.T

    def per_expert(total, inputs):
        gate_matrix, up_matrix, down_matrix, chosen, probs = inputs
        expert_rows = normed[chosen]
        gate_part = jnp.dot(expert_rows, gate_matrix, preferred_element_type=jnp.float32)
        up_part = jnp.dot(expert_rows, up_matrix, preferred_element_type=jnp.float32)
        hidden = (jax.nn.gelu(gate_part, approximate=True) * up_part).astype(jnp.bfloat16)
        expert_out = jnp.dot(hidden, down_matrix, preferred_element_type=jnp.float32).astype(jnp.bfloat16)
        weights = probs[chosen]
        total = total.at[chosen].add(weights[:, None] * expert_out.astype(jnp.float32))
        return (total, None)
    start = jnp.zeros(normed.shape, jnp.float32)
    total, unused = lax.scan(per_expert, start, (w_gate, w_up, w_down, selected.astype(jnp.int32), probs_by_expert))
    return total.astype(jnp.bfloat16)
```

```python
import functools

import jax
import jax.numpy as jnp
from jax import lax
from jax.experimental import pallas as pl
from jax.experimental.pallas import tpu as pltpu
from jax.sharding import PartitionSpec as P

F32, BF16, I32 = jnp.float32, jnp.bfloat16, jnp.int32
ANY = pl.BlockSpec(memory_space=pl.ANY)
VMEM = pl.BlockSpec(memory_space=pltpu.VMEM)
SMEM = pl.BlockSpec(memory_space=pltpu.SMEM)


def pack_kernel(order, slots, ids, tok, gain, router, sel, send, mix):
    rows, width = tok.shape
    experts = sel.shape[0]
    act = tok[...].astype(F32)
    scale = lax.rsqrt(jnp.mean(act * act, axis=1, keepdims=True) + 1e-06)
    normed = (act * scale * gain[...].astype(F32)).astype(BF16)
    logits = jnp.dot(normed, router[...], preferred_element_type=F32)
    gate = jax.nn.sigmoid(logits)
    gate_lane = lax.broadcasted_iota(I32, gate.shape, 1)
    base = ids[0] * rows
    token = base + lax.broadcasted_iota(I32, (rows, 1), 0)
    expert_row = lax.broadcasted_iota(I32, sel.shape, 0)
    lanes = lax.broadcasted_iota(I32, (rows, experts * slots), 1)
    target = jnp.full(lanes.shape, -1, I32)
    weight = jnp.zeros(lanes.shape, F32)
    for k, j in enumerate(order):
        row = lax.rem(ids[1] + j, experts)
        chosen = jnp.sum(jnp.where(expert_row == row, sel[...], 0), axis=0, keepdims=True)
        below = jnp.sum((chosen < token).astype(I32), axis=1, keepdims=True)
        taken = jnp.sum((chosen == token).astype(I32), axis=1, keepdims=True)
        rank = jnp.where(taken > 0, below - below[0:1], -1)
        prob = jnp.sum(jnp.where(gate_lane == row, gate, 0.0), axis=1, keepdims=True)
        here = lanes // slots == k
        target = jnp.where(here, rank, target)
        weight = jnp.where(here, prob, weight)
    hit = target == lanes % slots
    mix[...] = jnp.where(hit, weight, 0.0)
    onehot = jnp.where(hit, 1.0, 0.0).astype(BF16)
    send[...] = lax.dot_general(
        onehot, normed, (((0,), (0,)), ((), ())), preferred_element_type=F32
    ).astype(BF16)


def window_onehot(starts, counts, q, per, slots, window):
    first = starts[q * per]
    aligned = pl.multiple_of((first // 16) * 16, 16)
    lane = lax.broadcasted_iota(I32, (1, per * slots), 1)
    target = jnp.full(lane.shape, -1, I32)
    inside = lane % slots
    for b in range(per):
        here = (lane // slots == b) & (inside < counts[q * per + b])
        target = jnp.where(here, starts[q * per + b] - aligned + inside, target)
    place = lax.broadcasted_iota(I32, (window, per * slots), 0)
    return aligned, jnp.where(place == target, 1.0, 0.0).astype(BF16)


def mlp_kernel(n_in, per, slots, cap, starts, counts, *refs):
    ins = refs[:n_in]
    wg, wu, wd = refs[n_in : n_in + 3]
    outs = refs[n_in + 3 : 2 * n_in + 3]
    rows, acc, stage, in_sem, out_sem = refs[2 * n_in + 3 :]
    step = pl.program_id(0)
    block = per * slots
    window = block + 16

    @pl.when(step == 0)
    def _():
        def fetch(q):
            return pltpu.make_async_copy(ins[q], stage.at[q % 4], in_sem.at[q % 4])

        for q in range(min(3, n_in)):
            fetch(q).start()
        rows[...] = jnp.zeros(rows.shape, BF16)
        for q in range(n_in):
            fetch(q).wait()
            if q + 3 < n_in:
                fetch(q + 3).start()
            aligned, onehot = window_onehot(starts, counts, q, per, slots, window)
            part = jnp.dot(onehot, stage[q % 4], preferred_element_type=F32).astype(BF16)
            at = pl.ds(aligned, window)
            rows[at, :] = rows[at, :] + part

    x = rows[pl.ds(0, cap), :]
    up = jnp.dot(x, wu[0], preferred_element_type=F32)
    gated = jnp.dot(x, wg[0], preferred_element_type=F32)
    hidden = (jax.nn.gelu(gated, approximate=True) * up).astype(BF16)
    part = jnp.dot(hidden, wd[0], preferred_element_type=F32)

    @pl.when(step == 0)
    def _():
        acc[...] = part

    @pl.when(step > 0)
    def _():
        acc[...] += part

    @pl.when(step == pl.num_programs(0) - 1)
    def _():
        rows[pl.ds(0, cap), :] = acc[...].astype(BF16)

        def flush(q):
            return pltpu.make_async_copy(stage.at[q % 4], outs[q], out_sem.at[q % 4])

        for q in range(n_in):
            if q >= 4:
                flush(q - 4).wait()
            aligned, onehot = window_onehot(starts, counts, q, per, slots, window)
            stage[q % 4] = lax.dot_general(
                onehot,
                rows[pl.ds(aligned, window), :],
                (((0,), (0,)), ((), ())),
                preferred_element_type=F32,
            ).astype(BF16)
            flush(q).start()
        for q in range(max(0, n_in - 4), n_in):
            flush(q).wait()


def add_kernel(*refs):
    total = refs[0][...].astype(F32)
    for ref in refs[1:-1]:
        total = total + ref[...].astype(F32)
    refs[-1][...] = total.astype(BF16)


def add_blocks(blocks):
    size, width = blocks[0][2], blocks[0][0].shape[1]
    specs = [
        pl.BlockSpec((size, width), functools.partial(lambda n, i: (n, 0), n))
        for _, n, _ in blocks
    ]
    return pl.pallas_call(
        add_kernel,
        grid=(1,),
        in_specs=specs,
        out_specs=pl.BlockSpec((size, width), lambda i: (0, 0)),
        out_shape=jax.ShapeDtypeStruct((size, width), BF16),
    )(*[a for a, _, _ in blocks])


def mix_kernel(n_in, slots, mix, *refs):
    ins = refs[:n_in]
    out, held, sem = refs[n_in:]
    copies = [
        pltpu.make_async_copy(ins[k], held.at[pl.ds(k * slots, slots), :], sem.at[k])
        for k in range(n_in)
    ]
    for copy in copies:
        copy.start()
    weight = mix[...]
    high = weight.astype(BF16)
    low = (weight - high.astype(F32)).astype(BF16)
    for copy in copies:
        copy.wait()
    rows = held[...]
    total = jnp.dot(high, rows, preferred_element_type=F32)
    total = total + jnp.dot(low, rows, preferred_element_type=F32)
    out[...] = total.astype(BF16)


def per_device(tokens, norm_gain, router_weight, w_gate, w_up, w_down, selected):
    dp_count = lax.axis_size("dp")
    expert_count = lax.axis_size("expert")
    tok_rows, width = tokens.shape
    experts, cap = selected.shape
    slots = 4 * tok_rows // experts
    hidden_units = w_gate.shape[2]
    chips = dp_count // 2
    per = max(1, 128 // slots)
    block = per * slots
    order = sorted(range(expert_count), key=lambda j: (min(j, expert_count - j), j))
    groups = expert_count // per
    dp_index = lax.axis_index("dp")
    expert_index = lax.axis_index("expert")
    source = dp_index * expert_count + expert_index

    def over_expert(a, shift):
        pairs = [(s, (s + shift) % expert_count) for s in range(expert_count)]
        return lax.ppermute(a, "expert", pairs)

    def over_chips(a, shift):
        pairs = [(d, (d + 2 * shift) % dp_count) for d in range(dp_count)]
        return lax.ppermute(a, "dp", pairs)

    def swap_cores(a):
        return lax.ppermute(a, "dp", [(d, d ^ 1) for d in range(dp_count)])

    send, mix = pl.pallas_call(
        functools.partial(pack_kernel, order, slots),
        in_specs=[SMEM, VMEM, VMEM, VMEM, VMEM],
        out_specs=[VMEM, VMEM],
        out_shape=[
            jax.ShapeDtypeStruct((experts * slots, width), BF16),
            jax.ShapeDtypeStruct((tok_rows, experts * slots), F32),
        ],
    )(
        jnp.stack([source, expert_index]).astype(I32),
        tokens,
        norm_gain.reshape(1, width),
        router_weight,
        selected,
    )

    mine = lax.dynamic_index_in_dim(selected, expert_index, 0, keepdims=False)
    rel = jnp.arange(dp_count * expert_count, dtype=I32)
    far = rel // (2 * expert_count)
    other = (rel // expert_count) % 2
    shift = jnp.asarray(order, I32)[rel % expert_count]
    chip = (dp_index // 2 + chips - far) % chips
    core = (dp_index % 2 + other) % 2
    origin = (chip * 2 + core) * expert_count + (expert_index + expert_count - shift) % expert_count
    owner = mine // tok_rows
    counts = jnp.sum((owner[None, :] == origin[:, None]).astype(I32), axis=1)
    starts = jnp.sum(jnp.where(rel[None, :] < rel[:, None], counts[None, :], 0), axis=1)

    landed = {}
    for k, j in enumerate(order):
        piece = send[k * slots : (k + 1) * slots]
        landed[k] = over_expert(piece, j) if j else piece
    arrays = {}
    for n in range(groups):
        own = jnp.concatenate([landed[n * per + b] for b in range(per)], axis=0)
        arrays[0, 0, n] = own
        for far_by in range(1, chips):
            arrays[far_by, 0, n] = over_chips(own, far_by)
    for n in range(groups):
        for far_by in range(chips):
            arrays[far_by, 1, n] = swap_cores(arrays[far_by, 0, n])
    keys = [(f, c, n) for f in range(chips) for c in range(2) for n in range(groups)]
    n_in = len(keys)
    tile = 256 if hidden_units % 256 == 0 else 128
    outs = pl.pallas_call(
        functools.partial(mlp_kernel, n_in, per, slots, cap),
        grid=(hidden_units // tile,),
        in_specs=[SMEM, SMEM]
        + [ANY] * n_in
        + [
            pl.BlockSpec((1, width, tile), lambda i: (0, 0, i)),
            pl.BlockSpec((1, width, tile), lambda i: (0, 0, i)),
            pl.BlockSpec((1, tile, width), lambda i: (0, i, 0)),
        ],
        out_specs=[ANY] * n_in,
        out_shape=[jax.ShapeDtypeStruct((block, width), BF16)] * n_in,
        scratch_shapes=[
            pltpu.VMEM((cap + block + 16, width), BF16),
            pltpu.VMEM((cap, width), F32),
            pltpu.VMEM((4, block, width), BF16),
            pltpu.SemaphoreType.DMA((4,)),
            pltpu.SemaphoreType.DMA((4,)),
        ],
    )(starts, counts, *[arrays[key] for key in keys], w_gate, w_up, w_down)
    made = dict(zip(keys, outs))

    back = [None] * expert_count
    swapped = {}
    for n in reversed(range(groups)):
        for far_by in range(chips):
            swapped[far_by, n] = swap_cores(made[far_by, 1, n])
    for k in reversed(range(expert_count)):
        n, b = k // per, k % per
        parts = [(made[0, 0, n], b, slots), (swapped[0, n], b, slots)]
        for far_by in range(1, chips):
            pair = add_blocks([(made[far_by, 0, n], b, slots), (swapped[far_by, n], b, slots)])
            parts.append((over_chips(pair, chips - far_by), 0, slots))
        piece = add_blocks(parts)
        j = order[k]
        back[k] = over_expert(piece, expert_count - j) if j else piece

    return pl.pallas_call(
        functools.partial(mix_kernel, expert_count, slots),
        in_specs=[VMEM] + [ANY] * expert_count,
        out_specs=VMEM,
        out_shape=jax.ShapeDtypeStruct((tok_rows, width), BF16),
        scratch_shapes=[
            pltpu.VMEM((experts * slots, width), BF16),
            pltpu.SemaphoreType.DMA((expert_count,)),
        ],
    )(mix, *back)


def solution(mesh):
    in_specs = (
        P(("dp", "expert"), None),
        P(),
        P(),
        P("expert", None, "dp"),
        P("expert", None, "dp"),
        P("expert", "dp", None),
        P(),
    )
    out_specs = P(("dp", "expert"), None)
    return jax.shard_map(
        per_device, mesh=mesh, in_specs=in_specs, out_specs=out_specs, check_vma=False
    )
```
